32 devices in a mesh: path: 4 (over z), tm: 8 (over y, x, core).
Axes of the slice: x: 2, y: 2, z: 4, core: 2. Of those that a mesh axis runs over, the one named last changes fastest.
Arguments:
- values: bfloat16 [2048, 16, 2048], P('path', 'tm'), may hold values from -5 to 5
- hazard: float32 [16, 2048], P('tm', 'path'), may hold values from 0.0125 to 0.1875
- spread: float32 [16], P('tm'), may hold values from 0.3 to 3
- trade_set: int32 [2048], replicated, may hold values from 0 to 255
Outputs:
- pathwise_fva: float32 [2048, 256], P(('path', 'tm'))
- set_fva: float32 [256], P(('path', 'tm'))
The draws below stay inside these ranges and needn't reach their ends.
All inputs are finite; a program needn't handle non-finite values.
Results may differ from the reference program's by a relative error of at most 0.0003.
Values sent between devices are 32-bit elements; how exact they have to be, the bound alone decides.
A program may use at most 64 MiB of HBM per device.

```python
import math
import jax
import jax.numpy as jnp
from jax import lax

TRADES = 2048
SETS = 256
PATH_DEV = 512
PATHS = 2048
DATES = 16


def set_ends(result, rng, least, largest):
    extent = result.shape
    place = [jax.random.randint(jax.random.fold_in(rng, axis), (), 0, extent[axis]) for axis in range(len(extent))]
    result = result.at[tuple(place)].set(least)
    longest = extent.index(max(extent))
    place[longest] = (place[longest] + 1) % extent[longest]
    return result.at[tuple(place)].set(largest)


def block_levels(key, dims, shards, smallest, largest):
    gain, own = 1.0, jax.random.fold_in(key, 6)
    for axis_at, blocks in shards:
        draws = jnp.exp(jax.random.uniform(jax.random.fold_in(own, axis_at), (blocks,), jnp.float32, smallest / len(shards), largest / len(shards)))
        gain = gain * jnp.repeat(draws, dims[axis_at] // blocks).reshape([-1 if axis == axis_at else 1 for axis in range(len(dims))])
    return gain


def normal_values(own_key, shape, deviation, bound, shards=(), kind=jnp.bfloat16):
    result = jax.random.normal(own_key, shape, jnp.float32) * deviation
    if len(shards) > 0:
        result = block_levels(own_key, shape, shards, -0.22, 0.18) * result
    return jnp.clip(result, min=-bound, max=bound).astype(kind)


def setup_inputs(seed: int = 0) -> dict:
    keys = jax.random.split(jax.random.key(seed), 5)
    values = normal_values(keys[0], (PATHS, DATES, TRADES), 0.35, 5.0, ((0, 4), (1, 8)))
    hazard = jnp.clip(jnp.exp(math.log(0.1875) - 2.7080502 * jax.random.uniform(keys[1], (DATES, PATHS), jnp.float32) ** block_levels(keys[1], (DATES, PATHS), ((0, 8), (1, 4)), -0.2, 0.2)), 0.0125, 0.1875)
    spread = jnp.clip(jnp.exp(math.log(3.0) - 2.3025851 * jax.random.uniform(keys[2], (DATES,), jnp.float32) ** block_levels(keys[2], (DATES,), ((0, 8),), -0.2, 0.2)), 0.3, 3.0)
    trade_set = set_ends(jax.random.randint(keys[3], (TRADES,), 0, SETS), jax.random.fold_in(keys[3], 1), 0, SETS - 1).astype(jnp.int32)
    return dict(values=values, hazard=hazard, spread=spread, trade_set=trade_set)


def reference(values, hazard, spread, trade_set):
    onehot = (trade_set[:, None] == jnp.arange(SETS, dtype=jnp.int32)[None, :]).astype(jnp.bfloat16)
    survival = jnp.exp(-jnp.cumsum(hazard, axis=0))
    weights = spread[:, None] * survival
    blocks = PATHS // PATH_DEV
    value_blocks = values.reshape(blocks, PATH_DEV, DATES, TRADES)
    weight_blocks = jnp.transpose(weights.reshape(DATES, blocks, PATH_DEV), (1, 2, 0))

    def one_block(item):
        block_values, block_weights = item
        netted = jnp.dot(block_values.reshape(PATH_DEV * DATES, TRADES), onehot, preferred_element_type=jnp.float32)
        positive = jnp.maximum(netted.reshape(PATH_DEV, DATES, SETS), 0.0)
        return jnp.einsum("pt,pts->ps", block_weights, positive, precision=lax.Precision.HIGHEST)

    pathwise_fva = lax.map(one_block, (value_blocks, weight_blocks)).reshape(PATHS, SETS) / DATES
    set_fva = jnp.sum(pathwise_fva, axis=0) / PATHS
    return pathwise_fva, set_fva
```

```python
import functools

import jax
import jax.numpy as jnp
from jax import lax
from jax.experimental import pallas as pl
from jax.experimental.pallas import tpu as pltpu
from jax.sharding import PartitionSpec as P

SETS = 256
CHUNK_PATHS = 128
LANES = 128
MESH = pl.DeviceIdType.MESH


def kernel(
    n_path, n_tm, values, hazard_in, spread, trade_in, out, set_out,
    vbuf, ts, oh, hz, nbuf, wt, contrib, recv, hbuf, erow, ecol, setrow, setbuf,
    load_sem, small_sem, h_send, h_recv, b_send, b_recv, s_send, s_recv,
):
    paths, dates, trades = values.shape
    own = paths // n_tm
    chunks = paths // CHUNK_PATHS
    per = n_tm // chunks
    n_all = n_path * n_tm
    path_at, me = lax.axis_index("path"), lax.axis_index("tm")
    flat = path_at * n_tm + me
    rows = CHUNK_PATHS * dates
    my_chunk = lax.div(me, per)
    first = [lax.rem(my_chunk + 1 + i, chunks) for i in range(chunks)]
    flat_values = values.reshape(paths * dates, trades)

    def load(i):
        span = pl.ds(pl.multiple_of(first[i] * rows, rows), rows)
        return pltpu.make_async_copy(flat_values.at[span], vbuf.at[span], load_sem.at[i])

    copy_trades = pltpu.make_async_copy(trade_in, ts, small_sem.at[0])
    copy_hazard = pltpu.make_async_copy(hazard_in, hz, small_sem.at[1])
    copy_trades.start()
    copy_hazard.start()
    for i in range(chunks):
        load(i).start()

    barrier = pltpu.get_barrier_semaphore()

    def greet(k, carry):
        other = lax.rem(flat + k, n_all)
        pl.semaphore_signal(
            barrier, inc=1, device_id=(lax.div(other, n_tm), lax.rem(other, n_tm)), device_id_type=MESH
        )
        return carry

    lax.fori_loop(1, n_all, greet, 0)

    copy_trades.wait()
    set_at = lax.broadcasted_iota(jnp.int32, (SETS, LANES), 0)
    for block in range(trades // LANES):
        same = jnp.broadcast_to(ts[pl.ds(block, 1), :], (SETS, LANES)) == set_at
        oh[:, pl.ds(block * LANES, LANES)] = jnp.where(same, 1.0, 0.0).astype(jnp.bfloat16)

    copy_hazard.wait()
    total = jnp.zeros((1, paths), jnp.float32)
    weight_rows = []
    scale = 1.0 / (dates * n_tm)
    for d in range(dates):
        total = total + hz[pl.ds(d, 1), :]
        weight_rows.append((spread[d] * scale) * jnp.exp(-total))
    weight_rows.append(jnp.zeros((8 - dates, paths), jnp.float32))
    wt[...] = jnp.transpose(jnp.concatenate(weight_rows, axis=0))
    hbuf[me] = hz[...]

    def hazard_copy(other):
        return pltpu.make_async_remote_copy(
            src_ref=hz, dst_ref=hbuf.at[me], send_sem=h_send.at[other], recv_sem=h_recv.at[me],
            device_id=(path_at, other), device_id_type=MESH,
        )

    def hazard_arrival(other):
        return pltpu.make_async_remote_copy(
            src_ref=hz, dst_ref=hbuf.at[other], send_sem=h_send.at[other], recv_sem=h_recv.at[other],
            device_id=(path_at, other), device_id_type=MESH,
        )

    def own_rows(index):
        return pl.ds(pl.multiple_of(index * own, own), own)

    def block_copy(other):
        return pltpu.make_async_remote_copy(
            src_ref=contrib.at[own_rows(other)], dst_ref=recv.at[me],
            send_sem=b_send.at[other], recv_sem=b_recv.at[me],
            device_id=(path_at, other), device_id_type=MESH,
        )

    def block_arrival(other):
        return pltpu.make_async_remote_copy(
            src_ref=contrib.at[own_rows(other)], dst_ref=recv.at[other],
            send_sem=b_send.at[other], recv_sem=b_recv.at[other],
            device_id=(path_at, other), device_id_type=MESH,
        )

    peers = [lax.rem(me + k, n_tm) for k in range(1, n_tm)]
    for i in range(chunks):
        load(i).wait()
        span = pl.ds(pl.multiple_of(first[i] * rows, rows), rows)
        netted = lax.dot_general(
            vbuf[span, :], oh[...], (((1,), (1,)), ((), ())), preferred_element_type=jnp.float32
        )
        for h in range(SETS // LANES):
            nbuf[i, h] = netted[:, h * LANES : (h + 1) * LANES]
        path_span = pl.ds(pl.multiple_of(first[i] * CHUNK_PATHS, CHUNK_PATHS), CHUNK_PATHS)
        weight = wt[path_span, :]
        for h in range(SETS // LANES):
            part = None
            for d in range(dates):
                picked = nbuf[i, h, pl.ds(d, CHUNK_PATHS, stride=dates), :]
                term = weight[:, d : d + 1] * jnp.maximum(picked, 0.0)
                part = term if part is None else part + term
            contrib[path_span, pl.ds(h * LANES, LANES)] = part
        if i == 0:
            pl.semaphore_wait(barrier, n_all - 1)
            for other in peers:
                hazard_copy(other).start()
        if i < chunks - 1:
            for q in range(per):
                block_copy(first[i] * per + q).start()
        else:
            for q in range(1, per):
                block_copy(my_chunk * per + lax.rem(lax.rem(me, per) + q, per)).start()

    for other in peers:
        hazard_arrival(other).wait_recv()
    block_sums = jnp.sum(hbuf[...], axis=1)
    before = jnp.zeros((1, paths), jnp.float32)
    prefix = []
    for k in range(n_tm):
        prefix.append(before)
        before = before + block_sums[k : k + 1, :]
    earlier = jnp.exp(-jnp.concatenate(prefix, axis=0))
    erow[...] = earlier
    ecol[...] = jnp.transpose(earlier)
    mine = jnp.broadcast_to(erow[pl.ds(me, 1), :], (8, paths))
    set_part = jnp.dot(
        mine, contrib[...], precision=lax.Precision.HIGHEST, preferred_element_type=jnp.float32
    )
    setrow[...] = set_part[:1] * (1.0 / (paths * n_path))

    def set_copy(k, arrival):
        other = lax.rem(flat + k, n_all)
        slot = other if arrival else flat
        return pltpu.make_async_remote_copy(
            src_ref=setrow, dst_ref=setbuf.at[slot], send_sem=s_send.at[other], recv_sem=s_recv.at[slot],
            device_id=(lax.div(other, n_tm), lax.rem(other, n_tm)), device_id_type=MESH,
        )

    def send_set(k, carry):
        set_copy(k, False).start()
        return carry

    lax.fori_loop(1, n_all, send_set, 0)
    setbuf[flat] = setrow[...]

    recv[me] = contrib[own_rows(me), :]
    for other in peers:
        block_arrival(other).wait_recv()
    factor = ecol[own_rows(me), :]
    result = None
    for k in range(n_tm):
        term = factor[:, k : k + 1] * recv[k]
        result = term if result is None else result + term
    out[...] = result

    def take_set(k, carry):
        set_copy(k, True).wait_recv()
        return carry

    lax.fori_loop(1, n_all, take_set, 0)
    sums = jnp.broadcast_to(jnp.sum(setbuf[...], axis=0), (8, SETS))
    share = SETS // n_all
    turned = pltpu.roll(sums, lax.rem(SETS - flat * share, SETS), 1)
    set_out[...] = turned[:1, :share]

    for other in peers:
        hazard_copy(other).wait_send()
        block_copy(other).wait_send()

    def drain(k, carry):
        set_copy(k, False).wait_send()
        return carry

    lax.fori_loop(1, n_all, drain, 0)


def solution(mesh):
    n_path, n_tm = mesh.shape["path"], mesh.shape["tm"]
    n_all = n_path * n_tm

    def on_device(values, hazard, spread, trade_set):
        paths, dates, trades = values.shape
        own = paths // n_tm
        chunks = paths // CHUNK_PATHS
        f32 = jnp.float32
        any_space = pl.BlockSpec(memory_space=pltpu.HBM)
        vmem = pl.BlockSpec(memory_space=pltpu.VMEM)
        dma = pltpu.SemaphoreType.DMA
        pathwise, sets = pl.pallas_call(
            functools.partial(kernel, n_path, n_tm),
            out_shape=(
                jax.ShapeDtypeStruct((own, SETS), f32),
                jax.ShapeDtypeStruct((1, SETS // n_all), f32),
            ),
            in_specs=[any_space, any_space, pl.BlockSpec(memory_space=pltpu.SMEM), any_space],
            out_specs=(vmem, vmem),
            scratch_shapes=[
                pltpu.VMEM((paths * dates, trades), jnp.bfloat16),
                pltpu.VMEM((trades // LANES, LANES), jnp.int32),
                pltpu.VMEM((SETS, trades), jnp.bfloat16),
                pltpu.VMEM((dates, paths), f32),
                pltpu.VMEM((chunks, SETS // LANES, CHUNK_PATHS * dates, LANES), f32),
                pltpu.VMEM((paths, 8), f32),
                pltpu.VMEM((paths, SETS), f32),
                pltpu.VMEM((n_tm, own, SETS), f32),
                pltpu.VMEM((n_tm, dates, paths), f32),
                pltpu.VMEM((n_tm, paths), f32),
                pltpu.VMEM((paths, n_tm), f32),
                pltpu.VMEM((1, SETS), f32),
                pltpu.VMEM((n_all, 1, SETS), f32),
                dma((chunks,)),
                dma((2,)),
                dma((n_tm,)),
                dma((n_tm,)),
                dma((n_tm,)),
                dma((n_tm,)),
                dma((n_all,)),
                dma((n_all,)),
            ],
            compiler_params=pltpu.CompilerParams(
                collective_id=0, has_side_effects=True, vmem_limit_bytes=63 * 1024 * 1024
            ),
        )(values, hazard, spread, trade_set.reshape(trades // LANES, LANES))
        return pathwise, sets.reshape(SETS // n_all)

    in_specs = (P("path", "tm", None), P("tm", "path"), P("tm"), P())
    out_specs = (P(("path", "tm"), None), P(("path", "tm")))
    return jax.shard_map(
        on_device, mesh=mesh, in_specs=in_specs, out_specs=out_specs, check_vma=False
    )
```

```python
import functools

import jax
import jax.numpy as jnp
from jax import lax
from jax.experimental import pallas as pl
from jax.experimental.pallas import tpu as pltpu
from jax.sharding import PartitionSpec as P

SETS = 256
CHUNK_PATHS = 128
LANES = 128
MESH = pl.DeviceIdType.MESH


def kernel(
    n_path, n_tm, values, hazard_in, spread, trade_in, out, set_out,
    vbuf, ts, oh, hz, nbuf, wt, contrib, pair, comb, recv, hbuf, pcol, erow, ecol, row_a, row_b, rows_a, rows_b,
    load_sem, small_sem, h_send, h_recv, p_send, p_recv, b_send, b_recv, a_send, a_recv, z_send, z_recv,
):
    paths, dates, trades = values.shape
    own = paths // n_tm
    chunks = paths // CHUNK_PATHS
    per = n_tm // chunks
    n_all = n_path * n_tm
    chips = n_tm // 2
    path_at, me = lax.axis_index("path"), lax.axis_index("tm")
    flat = path_at * n_tm + me
    chip, core = lax.div(me, 2), lax.rem(me, 2)
    partner = me + 1 - 2 * core
    peers = [lax.rem(me + k, n_tm) for k in range(1, n_tm)]
    path_peers = [lax.rem(path_at + k, n_path) for k in range(1, n_path)]
    rows = CHUNK_PATHS * dates
    my_chunk = lax.div(me, per)
    first = [lax.rem(my_chunk + 1 + i, chunks) for i in range(chunks)]
    flat_values = values.reshape(paths * dates, trades)

    def load(i):
        span = pl.ds(pl.multiple_of(first[i] * rows, rows), rows)
        return pltpu.make_async_copy(flat_values.at[span], vbuf.at[span], load_sem.at[i])

    copy_trades = pltpu.make_async_copy(trade_in, ts, small_sem.at[0])
    copy_hazard = pltpu.make_async_copy(hazard_in, hz, small_sem.at[1])
    copy_trades.start()
    copy_hazard.start()
    for i in range(chunks):
        load(i).start()

    barrier = pltpu.get_barrier_semaphore()

    for other in peers:
        pl.semaphore_signal(barrier, inc=1, device_id=(path_at, other), device_id_type=MESH)
    for other in path_peers:
        pl.semaphore_signal(barrier, inc=1, device_id=(other, me), device_id_type=MESH)

    copy_trades.wait()
    set_at = lax.broadcasted_iota(jnp.int32, (SETS, LANES), 0)
    for block in range(trades // LANES):
        same = jnp.broadcast_to(ts[pl.ds(block, 1), :], (SETS, LANES)) == set_at
        oh[:, pl.ds(block * LANES, LANES)] = jnp.where(same, 1.0, 0.0).astype(jnp.bfloat16)

    copy_hazard.wait()
    total = jnp.zeros((1, paths), jnp.float32)
    weight_rows = []
    scale = 1.0 / (dates * n_tm)
    for d in range(dates):
        total = total + hz[pl.ds(d, 1), :]
        weight_rows.append((spread[d] * scale) * jnp.exp(-total))
    weight_rows.append(jnp.zeros((8 - dates, paths), jnp.float32))
    wt[...] = jnp.transpose(jnp.concatenate(weight_rows, axis=0))
    hbuf[me] = hz[...]

    def remote(src, dst, send, recv_at, device):
        return pltpu.make_async_remote_copy(
            src_ref=src, dst_ref=dst, send_sem=send, recv_sem=recv_at, device_id=device, device_id_type=MESH
        )

    def own_rows(index):
        return pl.ds(pl.multiple_of(index * own, own), own)

    def hazard_copy(other, slot):
        return remote(hz, hbuf.at[slot], h_send.at[other], h_recv.at[slot], (path_at, other))

    def pair_copy(q):
        theirs = contrib.at[own_rows(q * 2 + 1 - core)]
        return remote(theirs, pair.at[q], p_send.at[q], p_recv.at[q], (path_at, partner))

    def block_copy(q, slot):
        return remote(comb.at[q], recv.at[slot], b_send.at[q], b_recv.at[slot], (path_at, q * 2 + core))

    def plane_row(other, slot):
        return remote(row_a, rows_a.at[slot], a_send.at[other], a_recv.at[slot], (path_at, other))

    def path_row(other, slot):
        return remote(row_b, rows_b.at[slot], z_send.at[other], z_recv.at[slot], (other, me))

    def combine(q):
        pair_copy(q).wait_recv()
        mine = own_rows(q * 2 + core)
        factor = pcol[mine, :]
        return factor[:, 0:1] * contrib[mine, :] + factor[:, 1:2] * pair[q]

    def forward(i):
        for k in range(per // 2):
            q = first[i] * (per // 2) + k
            comb[q] = combine(q)
            block_copy(q, chip).start()

    for i in range(chunks):
        load(i).wait()
        span = pl.ds(pl.multiple_of(first[i] * rows, rows), rows)
        netted = lax.dot_general(
            vbuf[span, :], oh[...], (((1,), (1,)), ((), ())), preferred_element_type=jnp.float32
        )
        for h in range(SETS // LANES):
            nbuf[i, h] = netted[:, h * LANES : (h + 1) * LANES]
        path_span = pl.ds(pl.multiple_of(first[i] * CHUNK_PATHS, CHUNK_PATHS), CHUNK_PATHS)
        weight = wt[path_span, :]
        for h in range(SETS // LANES):
            part = None
            for d in range(dates):
                picked = nbuf[i, h, pl.ds(d, CHUNK_PATHS, stride=dates), :]
                term = weight[:, d : d + 1] * jnp.maximum(picked, 0.0)
                part = term if part is None else part + term
            contrib[path_span, pl.ds(h * LANES, LANES)] = part
        if i == 0:
            pl.semaphore_wait(barrier, n_tm - 1 + n_path - 1)
            hazard_copy(partner, me).start()
            for other in peers:
                @pl.when(other != partner)
                def _():
                    hazard_copy(other, me).start()
        for k in range(per // 2):
            pair_copy(first[i] * (per // 2) + k).start()
        if i == 1:
            hazard_copy(partner, partner).wait_recv()
            block = jnp.sum(hbuf[me - core], axis=0, keepdims=True)
            late = core.astype(jnp.float32)
            factors = [jnp.exp(-late * block), jnp.exp((late - 1.0) * block)]
            factors.append(jnp.zeros((6, paths), jnp.float32))
            pcol[...] = jnp.transpose(jnp.concatenate(factors, axis=0))
        if i >= 1:
            forward(i - 1)

    own_chips = [my_chunk * (per // 2) + lax.rem(lax.rem(chip, per // 2) + k, per // 2) for k in range(per // 2)]
    for q in own_chips[1:]:
        comb[q] = combine(q)
        block_copy(q, chip).start()

    for other in peers:
        @pl.when(other != partner)
        def _():
            hazard_copy(other, other).wait_recv()
    block_sums = jnp.sum(hbuf[...], axis=1)
    before = jnp.zeros((1, paths), jnp.float32)
    prefix = []
    for k in range(n_tm):
        prefix.append(before)
        before = before + block_sums[k : k + 1, :]
    earlier = jnp.exp(-jnp.concatenate(prefix, axis=0))
    erow[...] = earlier
    ecol[...] = jnp.transpose(earlier)
    mine = jnp.broadcast_to(erow[pl.ds(me, 1), :], (8, paths))
    set_part = jnp.dot(
        mine, contrib[...], precision=lax.Precision.HIGHEST, preferred_element_type=jnp.float32
    )
    row_a[...] = set_part[:1] * (1.0 / (paths * n_path))
    for other in peers:
        plane_row(other, me).start()
    rows_a[me] = row_a[...]
    recv[chip] = combine(own_chips[0])

    for other in peers:
        plane_row(other, other).wait_recv()
    row_b[...] = jnp.sum(rows_a[...], axis=0)
    for other in path_peers:
        path_row(other, path_at).start()
    rows_b[path_at] = row_b[...]

    other_chips = [lax.rem(chip + k, chips) for k in range(1, chips)]
    for q in other_chips:
        block_copy(q, q).wait_recv()
    factor = ecol[own_rows(me), :]
    result = None
    for k in range(chips):
        term = factor[:, 2 * k : 2 * k + 1] * recv[k]
        result = term if result is None else result + term
    out[...] = result

    for other in path_peers:
        path_row(other, other).wait_recv()
    sums = jnp.broadcast_to(jnp.sum(rows_b[...], axis=0), (8, SETS))
    share = SETS // n_all
    turned = pltpu.roll(sums, lax.rem(SETS - flat * share, SETS), 1)
    set_out[...] = turned[:1, :share]

    for other in peers:
        hazard_copy(other, me).wait_send()
        plane_row(other, me).wait_send()
    for other in path_peers:
        path_row(other, path_at).wait_send()
    for q in other_chips:
        pair_copy(q).wait_send()
        block_copy(q, chip).wait_send()
    pair_copy(chip).wait_send()


def finish(pathwise, sets, pathwise_out, sets_out):
    pathwise_out[...] = pathwise[...]
    sets_out[...] = sets[...]


def solution(mesh):
    n_path, n_tm = mesh.shape["path"], mesh.shape["tm"]
    n_all = n_path * n_tm

    def on_device(values, hazard, spread, trade_set):
        paths, dates, trades = values.shape
        own = paths // n_tm
        chunks = paths // CHUNK_PATHS
        f32 = jnp.float32
        any_space = pl.BlockSpec(memory_space=pltpu.HBM)
        vmem = pl.BlockSpec(memory_space=pltpu.VMEM)
        dma = pltpu.SemaphoreType.DMA
        pathwise, sets = pl.pallas_call(
            functools.partial(kernel, n_path, n_tm),
            out_shape=(
                jax.ShapeDtypeStruct((own, SETS), f32),
                jax.ShapeDtypeStruct((1, SETS // n_all), f32),
            ),
            in_specs=[any_space, any_space, pl.BlockSpec(memory_space=pltpu.SMEM), any_space],
            out_specs=(vmem, vmem),
            scratch_shapes=[
                pltpu.VMEM((paths * dates, trades), jnp.bfloat16),
                pltpu.VMEM((trades // LANES, LANES), jnp.int32),
                pltpu.VMEM((SETS, trades), jnp.bfloat16),
                pltpu.VMEM((dates, paths), f32),
                pltpu.VMEM((chunks, SETS // LANES, CHUNK_PATHS * dates, LANES), f32),
                pltpu.VMEM((paths, 8), f32),
                pltpu.VMEM((paths, SETS), f32),
                pltpu.VMEM((n_tm // 2, own, SETS), f32),
                pltpu.VMEM((n_tm // 2, own, SETS), f32),
                pltpu.VMEM((n_tm // 2, own, SETS), f32),
                pltpu.VMEM((n_tm, dates, paths), f32),
                pltpu.VMEM((paths, 8), f32),
                pltpu.VMEM((n_tm, paths), f32),
                pltpu.VMEM((paths, n_tm), f32),
                pltpu.VMEM((1, SETS), f32),
                pltpu.VMEM((1, SETS), f32),
                pltpu.VMEM((n_tm, 1, SETS), f32),
                pltpu.VMEM((n_path, 1, SETS), f32),
                dma((chunks,)),
                dma((2,)),
                dma((n_tm,)),
                dma((n_tm,)),
                dma((n_tm // 2,)),
                dma((n_tm // 2,)),
                dma((n_tm // 2,)),
                dma((n_tm // 2,)),
                dma((n_tm,)),
                dma((n_tm,)),
                dma((n_path,)),
                dma((n_path,)),
            ],
            compiler_params=pltpu.CompilerParams(
                collective_id=0, has_side_effects=True, vmem_limit_bytes=62 * 1024 * 1024
            ),
        )(values, hazard, spread, trade_set.reshape(trades // LANES, LANES))
        pathwise, sets = pl.pallas_call(
            finish,
            out_shape=(
                jax.ShapeDtypeStruct(pathwise.shape, f32),
                jax.ShapeDtypeStruct(sets.shape, f32),
            ),
            in_specs=[vmem, vmem],
            out_specs=(vmem, vmem),
        )(pathwise, sets)
        return pathwise, sets.reshape(SETS // n_all)

    in_specs = (P("path", "tm", None), P("tm", "path"), P("tm"), P())
    out_specs = (P(("path", "tm"), None), P(("path", "tm")))
    return jax.shard_map(
        on_device, mesh=mesh, in_specs=in_specs, out_specs=out_specs, check_vma=False
    )
```

```python
import functools

import jax
import jax.numpy as jnp
from jax import lax
from jax.experimental import pallas as pl
from jax.experimental.pallas import tpu as pltpu
from jax.sharding import PartitionSpec as P

SETS = 256
CHUNK_PATHS = 128
LANES = 128
MESH = pl.DeviceIdType.MESH


def kernel(
    n_path, n_tm, values, hazard_in, spread, trade_in, out, set_out,
    vbuf, ts, oh, hz, nbuf, wt, contrib, pair, comb, recv, hbuf, pcol, erow, ecol, row_a, rows_a,
    load_sem, small_sem, h_send, h_recv, p_send, p_recv, b_send, b_recv, a_send, a_recv, ready,
):
    paths, dates, trades = values.shape
    own = paths // n_tm
    chunks = paths // CHUNK_PATHS
    per = n_tm // chunks
    n_all = n_path * n_tm
    chips = n_tm // 2
    path_at, me = lax.axis_index("path"), lax.axis_index("tm")
    flat = path_at * n_tm + me
    chip, core = lax.div(me, 2), lax.rem(me, 2)
    partner = me + 1 - 2 * core
    peers = [lax.rem(me + k, n_tm) for k in range(1, n_tm)]
    path_peers = [lax.rem(path_at + k, n_path) for k in range(1, n_path)]
    rows = CHUNK_PATHS * dates
    my_chunk = lax.div(me, per)
    first = [lax.rem(my_chunk + 1 + i, chunks) for i in range(chunks)]
    flat_values = values.reshape(paths * dates, trades)

    def load(i):
        span = pl.ds(pl.multiple_of(first[i] * rows, rows), rows)
        return pltpu.make_async_copy(flat_values.at[span], vbuf.at[span], load_sem.at[i])

    copy_trades = pltpu.make_async_copy(trade_in, ts, small_sem.at[0])
    copy_hazard = pltpu.make_async_copy(hazard_in, hz, small_sem.at[1])
    copy_trades.start()
    copy_hazard.start()
    for i in range(chunks):
        load(i).start()

    barrier = pltpu.get_barrier_semaphore()

    for other in peers:
        pl.semaphore_signal(barrier, inc=1, device_id=(path_at, other), device_id_type=MESH)
    for other in path_peers:
        pl.semaphore_signal(barrier, inc=1, device_id=(other, me), device_id_type=MESH)

    copy_trades.wait()
    set_at = lax.broadcasted_iota(jnp.int32, (SETS, LANES), 0)
    for block in range(trades // LANES):
        same = jnp.broadcast_to(ts[pl.ds(block, 1), :], (SETS, LANES)) == set_at
        oh[:, pl.ds(block * LANES, LANES)] = jnp.where(same, 1.0, 0.0).astype(jnp.bfloat16)

    copy_hazard.wait()
    total = jnp.zeros((1, paths), jnp.float32)
    weight_rows = []
    scale = 1.0 / (dates * n_tm)
    for d in range(dates):
        total = total + hz[pl.ds(d, 1), :]
        weight_rows.append((spread[d] * scale) * jnp.exp(-total))
    weight_rows.append(jnp.zeros((8 - dates, paths), jnp.float32))
    wt[...] = jnp.transpose(jnp.concatenate(weight_rows, axis=0))
    hbuf[me] = hz[...]

    def remote(src, dst, send, recv_at, device):
        return pltpu.make_async_remote_copy(
            src_ref=src, dst_ref=dst, send_sem=send, recv_sem=recv_at, device_id=device, device_id_type=MESH
        )

    def own_rows(index):
        return pl.ds(pl.multiple_of(index * own, own), own)

    def hazard_copy(other, slot):
        return remote(hz, hbuf.at[slot], h_send.at[other], h_recv.at[slot], (path_at, other))

    def pair_copy(q):
        theirs = contrib.at[own_rows(q * 2 + 1 - core)]
        return remote(theirs, pair.at[q], p_send.at[q], p_recv.at[q], (path_at, partner))

    def block_copy(q, slot):
        return remote(comb.at[q], recv.at[slot], b_send.at[q], b_recv.at[slot], (path_at, q * 2 + core))

    targets = [(z, other) for z in path_peers for other in peers + [me]]
    targets += [(path_at, other) for other in peers]

    def set_row(z, other, slot):
        return remote(row_a, rows_a.at[slot], a_send.at[z * n_tm + other], a_recv.at[slot], (z, other))

    def combine(q):
        pair_copy(q).wait_recv()
        mine = own_rows(q * 2 + core)
        factor = pcol[mine, :]
        return factor[:, 0:1] * contrib[mine, :] + factor[:, 1:2] * pair[q]

    def forward(i):
        for k in range(per // 2):
            q = first[i] * (per // 2) + k
            comb[q] = combine(q)
            block_copy(q, chip).start()

    for i in range(chunks):
        load(i).wait()
        span = pl.ds(pl.multiple_of(first[i] * rows, rows), rows)
        netted = lax.dot_general(
            vbuf[span, :], oh[...], (((1,), (1,)), ((), ())), preferred_element_type=jnp.float32
        )
        for h in range(SETS // LANES):
            nbuf[i, h] = netted[:, h * LANES : (h + 1) * LANES]
        path_span = pl.ds(pl.multiple_of(first[i] * CHUNK_PATHS, CHUNK_PATHS), CHUNK_PATHS)
        weight = wt[path_span, :]
        for h in range(SETS // LANES):
            part = None
            for d in range(dates):
                picked = nbuf[i, h, pl.ds(d, CHUNK_PATHS, stride=dates), :]
                term = weight[:, d : d + 1] * jnp.maximum(picked, 0.0)
                part = term if part is None else part + term
            contrib[path_span, pl.ds(h * LANES, LANES)] = part
        if i == 0:
            pl.semaphore_wait(barrier, n_tm - 1 + n_path - 1)
            for other in path_peers:
                pl.semaphore_signal(ready, inc=1, device_id=(other, me), device_id_type=MESH)
            hazard_copy(partner, me).start()
            for other in peers:
                @pl.when(other != partner)
                def _():
                    hazard_copy(other, me).start()
        for k in range(per // 2):
            pair_copy(first[i] * (per // 2) + k).start()
        if i == 1:
            hazard_copy(partner, partner).wait_recv()
            block = jnp.sum(hbuf[me - core], axis=0, keepdims=True)
            late = core.astype(jnp.float32)
            factors = [jnp.exp(-late * block), jnp.exp((late - 1.0) * block)]
            factors.append(jnp.zeros((6, paths), jnp.float32))
            pcol[...] = jnp.transpose(jnp.concatenate(factors, axis=0))
        if 1 <= i < chunks - 1:
            forward(i - 1)

    for other in peers:
        @pl.when(other != partner)
        def _():
            hazard_copy(other, other).wait_recv()
    block_sums = jnp.sum(hbuf[...], axis=1)
    before = jnp.zeros((1, paths), jnp.float32)
    prefix = []
    for k in range(n_tm):
        prefix.append(before)
        before = before + block_sums[k : k + 1, :]
    earlier = jnp.exp(-jnp.concatenate(prefix, axis=0))
    erow[...] = earlier
    ecol[...] = jnp.transpose(earlier)
    mine = jnp.broadcast_to(erow[pl.ds(me, 1), :], (8, paths))
    set_part = jnp.dot(
        mine, contrib[...], precision=lax.Precision.HIGHEST, preferred_element_type=jnp.float32
    )
    row_a[...] = set_part[:1] * (1.0 / (paths * n_path))
    pl.semaphore_wait(ready, n_path - 1)
    for z, other in targets:
        set_row(z, other, flat).start()
    forward(chunks - 2)
    own_chips = [my_chunk * (per // 2) + lax.rem(lax.rem(chip, per // 2) + k, per // 2) for k in range(per // 2)]
    for q in own_chips[1:]:
        comb[q] = combine(q)
        block_copy(q, chip).start()

    rows_a[flat] = row_a[...]
    recv[chip] = combine(own_chips[0])

    other_chips = [lax.rem(chip + k, chips) for k in range(1, chips)]
    for q in other_chips:
        block_copy(q, q).wait_recv()
    factor = ecol[own_rows(me), :]
    result = None
    for k in range(chips):
        term = factor[:, 2 * k : 2 * k + 1] * recv[k]
        result = term if result is None else result + term
    out[...] = result

    for z, other in targets:
        set_row(z, other, z * n_tm + other).wait_recv()
    sums = jnp.broadcast_to(jnp.sum(rows_a[...], axis=0), (8, SETS))
    share = SETS // n_all
    turned = pltpu.roll(sums, lax.rem(SETS - flat * share, SETS), 1)
    set_out[...] = turned[:1, :share]

    for other in peers:
        hazard_copy(other, me).wait_send()
    for z, other in targets:
        set_row(z, other, flat).wait_send()
    for q in other_chips:
        pair_copy(q).wait_send()
        block_copy(q, chip).wait_send()
    pair_copy(chip).wait_send()


def finish(pathwise, sets, pathwise_out, sets_out):
    pathwise_out[...] = pathwise[...]
    sets_out[...] = sets[...]


def solution(mesh):
    n_path, n_tm = mesh.shape["path"], mesh.shape["tm"]
    n_all = n_path * n_tm

    def on_device(values, hazard, spread, trade_set):
        paths, dates, trades = values.shape
        own = paths // n_tm
        chunks = paths // CHUNK_PATHS
        f32 = jnp.float32
        any_space = pl.BlockSpec(memory_space=pltpu.HBM)
        vmem = pl.BlockSpec(memory_space=pltpu.VMEM)
        dma = pltpu.SemaphoreType.DMA
        pathwise, sets = pl.pallas_call(
            functools.partial(kernel, n_path, n_tm),
            out_shape=(
                jax.ShapeDtypeStruct((own, SETS), f32),
                jax.ShapeDtypeStruct((1, SETS // n_all), f32),
            ),
            in_specs=[any_space, any_space, pl.BlockSpec(memory_space=pltpu.SMEM), any_space],
            out_specs=(vmem, vmem),
            scratch_shapes=[
                pltpu.VMEM((paths * dates, trades), jnp.bfloat16),
                pltpu.VMEM((trades // LANES, LANES), jnp.int32),
                pltpu.VMEM((SETS, trades), jnp.bfloat16),
                pltpu.VMEM((dates, paths), f32),
                pltpu.VMEM((chunks, SETS // LANES, CHUNK_PATHS * dates, LANES), f32),
                pltpu.VMEM((paths, 8), f32),
                pltpu.VMEM((paths, SETS), f32),
                pltpu.VMEM((n_tm // 2, own, SETS), f32),
                pltpu.VMEM((n_tm // 2, own, SETS), f32),
                pltpu.VMEM((n_tm // 2, own, SETS), f32),
                pltpu.VMEM((n_tm, dates, paths), f32),
                pltpu.VMEM((paths, 8), f32),
                pltpu.VMEM((n_tm, paths), f32),
                pltpu.VMEM((paths, n_tm), f32),
                pltpu.VMEM((1, SETS), f32),
                pltpu.VMEM((n_all, 1, SETS), f32),
                dma((chunks,)),
                dma((2,)),
                dma((n_tm,)),
                dma((n_tm,)),
                dma((n_tm // 2,)),
                dma((n_tm // 2,)),
                dma((n_tm // 2,)),
                dma((n_tm // 2,)),
                dma((n_all,)),
                dma((n_all,)),
                pltpu.SemaphoreType.REGULAR,
            ],
            compiler_params=pltpu.CompilerParams(
                collective_id=0, has_side_effects=True, vmem_limit_bytes=62 * 1024 * 1024
            ),
        )(values, hazard, spread, trade_set.reshape(trades // LANES, LANES))
        pathwise, sets = pl.pallas_call(
            finish,
            out_shape=(
                jax.ShapeDtypeStruct(pathwise.shape, f32),
                jax.ShapeDtypeStruct(sets.shape, f32),
            ),
            in_specs=[vmem, vmem],
            out_specs=(vmem, vmem),
        )(pathwise, sets)
        return pathwise, sets.reshape(SETS // n_all)

    in_specs = (P("path", "tm", None), P("tm", "path"), P("tm"), P())
    out_specs = (P(("path", "tm"), None), P(("path", "tm")))
    return jax.shard_map(
        on_device, mesh=mesh, in_specs=in_specs, out_specs=out_specs, check_vma=False
    )
```
